32 devices in a mesh: grp: 4 (over y, x), tp: 8 (over z, core).
Axes of the slice: x: 2, y: 2, z: 4, core: 2. Of those that a mesh axis runs over, the one named last changes fastest.
Arguments:
- tokens: bfloat16 [1280, 4096], P(('grp', 'tp')), may hold values from -6 to 6
- norm_gain: float32 [4096], replicated, may hold values from 0.5 to 1.5
- spill_blocks: int32 [1], replicated, may hold values from 0 to 7, as said below
- image_gate: bfloat16 [4096, 11008], P('grp', 'tp'), may hold values from -0.09375 to 0.09375
- image_up: bfloat16 [4096, 11008], P('grp', 'tp'), may hold values from -0.09375 to 0.09375
- image_down: bfloat16 [11008, 4096], P('tp', 'grp'), may hold values from -0.0546875 to 0.0546875
- text_gate: bfloat16 [4096, 11008], P(None, 'tp'), may hold values from -0.09375 to 0.09375
- text_up: bfloat16 [4096, 11008], P(None, 'tp'), may hold values from -0.09375 to 0.09375
- text_down: bfloat16 [11008, 4096], P('tp'), may hold values from -0.0546875 to 0.0546875
Outputs:
- mixed: bfloat16 [1280, 4096], P(('grp', 'tp'))
The draws below stay inside these ranges and needn't reach their ends.
Inputs may be any that keep to these rules, and one draw needn't show every extreme that they name: `spill_blocks`: 1 distinct indices of 0 to 8 - 1, in increasing order.
All inputs are finite; a program needn't handle non-finite values.
Results may differ from the reference program's by a relative error of at most 0.0046.
Values may be sent and summed in bfloat16 or wider, within the bound.
A program may use at most 256 MiB of HBM per device.

```python
import jax
import jax.numpy as jnp
from jax import lax

D = 4096
FF = 11008
TOK_DEV = 40
SPILL = 1
TOKENS = 1280
N_GRP = 4
N_TP = 8


def draw_spill_blocks(key, part):
    order = jax.random.permutation(jax.random.fold_in(key, 7), N_TP)
    return jnp.sort(order[:SPILL]).astype(jnp.int32)


def steps_of(stream_key, extent, pieces, low, top_value):
    level, own = 1.0, jax.random.fold_in(stream_key, 6)
    for position, parts in pieces:
        draws = jnp.exp(jax.random.uniform(jax.random.fold_in(own, position), (parts,), jnp.float32, low / len(pieces), top_value / len(pieces)))
        level = level * jnp.repeat(draws, extent[position] // parts).reshape([-1 if axis == position else 1 for axis in range(len(extent))])
    return level


def centred(stream_key, extent, spread, most, pieces=(), kind=jnp.bfloat16):
    factor_of = steps_of(stream_key, extent, pieces, -0.22, 0.18) if pieces else 1.0
    values = jax.random.normal(stream_key, extent, jnp.float32) * spread * factor_of
    return jnp.minimum(jnp.maximum(values, -most), most).astype(kind)


def setup_inputs(seed: int = 0) -> dict:
    arg_keys = jax.random.split(jax.random.key(seed), 10)
    tokens = centred(arg_keys[0], (TOKENS, D), 1.0, 6.0, ((0, 32),))
    norm_gain = jnp.clip(1.0 + 0.1 * jax.random.normal(arg_keys[1], (D,), jnp.float32), 0.5, 1.5)
    spill_blocks = draw_spill_blocks(jax.random.fold_in(arg_keys[9], 71), 0)
    image_gate = centred(arg_keys[3], (D, FF), D ** -0.5, 0.09375, ((0, 4), (1, 8)))
    image_up = centred(arg_keys[4], (D, FF), D ** -0.5, 0.09375, ((0, 4), (1, 8)))
    image_down = centred(arg_keys[5], (FF, D), FF ** -0.5, 0.0546875, ((0, 8), (1, 4)))
    text_gate = centred(arg_keys[6], (D, FF), D ** -0.5, 0.09375, ((1, 8),))
    text_up = centred(arg_keys[7], (D, FF), D ** -0.5, 0.09375, ((1, 8),))
    text_down = centred(arg_keys[8], (FF, D), FF ** -0.5, 0.0546875, ((0, 8),))
    return dict(tokens=tokens, norm_gain=norm_gain, spill_blocks=spill_blocks, image_gate=image_gate, image_up=image_up, image_down=image_down, text_gate=text_gate, text_up=text_up, text_down=text_down)


norm_epsilon = 1e-05

def feed_forward(inputs, w_gate, w_up, w_down):
    gate_out = jnp.dot(inputs, w_gate, preferred_element_type=jnp.float32)
    up_out = jnp.dot(inputs, w_up, preferred_element_type=jnp.float32)
    hidden = (jax.nn.silu(gate_out) * up_out).astype(jnp.bfloat16)
    return jnp.dot(hidden, w_down, preferred_element_type=jnp.float32)

def reference(tokens, norm_gain, spill_blocks, image_gate, image_up, image_down, text_gate, text_up, text_down):
    model_width = tokens.shape[1]
    tokens_wide = tokens.astype(jnp.float32)
    scale = lax.rsqrt(lax.optimization_barrier(jnp.mean(tokens_wide * tokens_wide, axis=-1, keepdims=True)) + norm_epsilon)
    normed = (tokens_wide * scale * norm_gain).astype(jnp.bfloat16)
    blocks = normed.reshape(N_GRP * N_TP, TOK_DEV, model_width)
    image_count = (N_GRP - 1) * N_TP
    text_part = blocks[image_count:]
    spill_mask = jnp.any(jnp.arange(N_TP, dtype=jnp.int32)[:, None] == spill_blocks[None, :], axis=1)
    text_ids = jnp.nonzero(jnp.logical_not(spill_mask), size=N_TP - SPILL)[0].astype(jnp.int32)
    image_rows = jnp.concatenate([blocks[:image_count], text_part[spill_blocks]], axis=0).reshape(-1, model_width)
    text_rows = text_part[text_ids].reshape(-1, model_width)
    image_out = feed_forward(image_rows, image_gate, image_up, image_down).reshape(-1, TOK_DEV, model_width)
    text_out = feed_forward(text_rows, text_gate, text_up, text_down).reshape(-1, TOK_DEV, model_width)
    text_branch = jnp.zeros((N_TP, TOK_DEV, model_width), jnp.float32)
    text_branch = text_branch.at[spill_blocks].set(image_out[image_count:]).at[text_ids].set(text_out)
    branch = jnp.concatenate([image_out[:image_count], text_branch], axis=0).reshape(-1, model_width)
    return (tokens_wide + branch).astype(jnp.bfloat16)
```

```python
import jax
import jax.numpy as jnp
from jax import lax
from jax.sharding import PartitionSpec as P

norm_epsilon = 1e-05
bf16 = jnp.bfloat16
f32 = jnp.float32


def on_device(
    tokens, norm_gain, spill_blocks, image_gate, image_up, image_down, text_gate, text_up, text_down
):
    rows, width = tokens.shape
    n_tp = lax.axis_size("tp")
    n_grp = lax.axis_size("grp")
    group = lax.axis_index("grp")
    n_spill = spill_blocks.shape[0]
    in_text = group == n_grp - 1
    kslice = image_gate.shape[0]
    units = image_gate.shape[1]
    wide = tokens.astype(f32)
    scale = lax.rsqrt(jnp.mean(wide * wide, axis=-1, keepdims=True) + norm_epsilon)
    normed = (wide * scale * norm_gain).astype(bf16)

    cols = normed.reshape(rows, n_grp, kslice).transpose(1, 0, 2)
    cols = lax.all_to_all(cols, "grp", 0, 0, tiled=True)
    cols = lax.all_gather(cols, "tp", axis=1, tiled=False)
    image_part = cols[: n_grp - 1].reshape(-1, kslice)
    spill_part = cols[n_grp - 1][spill_blocks].reshape(-1, kslice)
    x = jnp.concatenate([image_part, spill_part], axis=0)
    n_rows = x.shape[0]
    step = 16 * n_grp
    padded = (n_rows + step - 1) // step * step
    x = jnp.pad(x, ((0, padded - n_rows), (0, 0)))
    part_gate = jnp.dot(x, image_gate, preferred_element_type=f32).astype(bf16)
    part_up = jnp.dot(x, image_up, preferred_element_type=f32).astype(bf16)
    gate = lax.psum_scatter(part_gate, "grp", scatter_dimension=0, tiled=True)
    up = lax.psum_scatter(part_up, "grp", scatter_dimension=0, tiled=True)

    piece = lax.all_gather(normed, "tp", axis=0, tiled=True)

    def text_ffn():
        g = jnp.dot(piece, text_gate, preferred_element_type=f32)
        u = jnp.dot(piece, text_up, preferred_element_type=f32)
        h = (jax.nn.silu(g) * u).astype(bf16)
        return jnp.dot(h, text_down, preferred_element_type=f32).astype(bf16)

    text_terms = lax.cond(
        in_text, text_ffn, lambda: jnp.zeros((n_tp * rows, width), bf16)
    )
    text_out = lax.psum_scatter(text_terms, "tp", scatter_dimension=0, tiled=True)

    hidden = (jax.nn.silu(gate.astype(f32)) * up.astype(f32)).astype(bf16)
    hidden = lax.all_gather(hidden, "grp", axis=0, tiled=True)
    terms = jnp.dot(hidden, image_down, preferred_element_type=f32).astype(bf16)
    image_terms = terms[: (n_grp - 1) * n_tp * rows].reshape(n_grp - 1, n_tp, rows, kslice)
    spill_terms = terms[(n_grp - 1) * n_tp * rows : n_rows].reshape(n_spill, rows, kslice)
    placed = jnp.zeros((n_tp, rows, kslice), bf16).at[spill_blocks].set(spill_terms)
    every = jnp.concatenate([image_terms, placed[None]], axis=0).transpose(1, 0, 2, 3)
    mine = lax.psum_scatter(every.reshape(n_tp, -1, kslice), "tp", scatter_dimension=0, tiled=True)
    mine = mine.reshape(n_grp, rows, kslice)
    back = lax.all_to_all(mine, "grp", 0, 0, tiled=True)
    branch = back.transpose(1, 0, 2).reshape(rows, width)
    is_spill = jnp.any(lax.axis_index("tp") == spill_blocks)
    use_text = jnp.logical_and(in_text, jnp.logical_not(is_spill))
    branch = jnp.where(use_text, text_out, branch)
    return (wide + branch.astype(f32)).astype(bf16)


def solution(mesh):
    in_specs = (
        P(("grp", "tp"), None),
        P(),
        P(),
        P("grp", "tp"),
        P("grp", "tp"),
        P("tp", "grp"),
        P(None, "tp"),
        P(None, "tp"),
        P("tp", None),
    )
    out_specs = P(("grp", "tp"), None)
    return jax.shard_map(
        on_device, mesh=mesh, in_specs=in_specs, out_specs=out_specs, check_vma=False
    )
```

```python
import jax
import jax.numpy as jnp
from jax import lax
from jax.experimental import pallas as pl
from jax.experimental.pallas import tpu as pltpu
from jax.sharding import PartitionSpec as P

norm_epsilon = 1e-05
bf16 = jnp.bfloat16
f32 = jnp.float32

MESH = pl.DeviceIdType.MESH
chunk_count = 2


def plane_kernel(
    n,
    x_hbm,
    gate_hbm,
    up_hbm,
    down_hbm,
    out_ref,
    x,
    gate,
    up,
    down,
    part,
    own,
    landed,
    hidden,
    load_sem,
    part_send,
    part_recv,
    hid_send,
    hid_recv,
):
    me = lax.axis_index("grp")
    rows = part.shape[3]
    loads = [
        pltpu.make_async_copy(src, dst, load_sem.at[i])
        for i, (src, dst) in enumerate(
            ((x_hbm, x), (gate_hbm, gate), (up_hbm, up), (down_hbm, down))
        )
    ]
    for load in loads:
        load.start()
    barrier = pltpu.get_barrier_semaphore()
    for k in range(1, n):
        pl.semaphore_signal(
            barrier, inc=1, device_id={"grp": lax.rem(me + k, n)}, device_id_type=MESH
        )
    pl.semaphore_wait(barrier, n - 1)

    def part_copy(d, src_slot, dst_slot, c):
        return pltpu.make_async_remote_copy(
            src_ref=part.at[src_slot, c],
            dst_ref=landed.at[dst_slot, c],
            send_sem=part_send.at[src_slot, c],
            recv_sem=part_recv.at[dst_slot, c],
            device_id={"grp": d},
            device_id_type=MESH,
        )

    def hid_copy(d, owner, c):
        return pltpu.make_async_remote_copy(
            src_ref=hidden.at[owner, c],
            dst_ref=hidden.at[owner, c],
            send_sem=hid_send.at[d, c],
            recv_sem=hid_recv.at[owner, c],
            device_id={"grp": d},
            device_id_type=MESH,
        )

    def peer(k):
        return lax.rem(me + k, n)

    loads[0].wait()
    loads[1].wait()
    loads[2].wait()

    def send_step(s, carry):
        c = s // (n - 1)
        d = peer(n - 1 - s % (n - 1))
        block = x[d, c]
        part[d, c, 0] = jnp.dot(block, gate[...], preferred_element_type=f32).astype(bf16)
        part[d, c, 1] = jnp.dot(block, up[...], preferred_element_type=f32).astype(bf16)
        part_copy(d, d, me, c).start()
        return carry

    lax.fori_loop(0, chunk_count * (n - 1), send_step, 0)

    def own_step(c, carry):
        block = x[me, c]
        own[c, 0] = jnp.dot(block, gate[...], preferred_element_type=f32)
        own[c, 1] = jnp.dot(block, up[...], preferred_element_type=f32)
        return carry

    lax.fori_loop(0, chunk_count, own_step, 0)
    loads[3].wait()

    def hidden_step(c, carry):
        for k in range(1, n):
            part_copy(peer(k), peer(k), peer(k), c).wait_recv()

        def tile(r, inner):
            at = pl.ds(pl.multiple_of(r * 16, 16), 16)
            g = own[c, 0, at, :]
            u = own[c, 1, at, :]
            for k in range(1, n):
                g = g + landed[peer(k), c, 0, at, :].astype(f32)
                u = u + landed[peer(k), c, 1, at, :].astype(f32)
            hidden[me, c, at, :] = (g / (1.0 + jnp.exp(-g)) * u).astype(bf16)
            return inner

        lax.fori_loop(0, rows // 16, tile, 0)
        for k in range(n - 1, 0, -1):
            hid_copy(peer(k), me, c).start()
        return carry

    lax.fori_loop(0, chunk_count, hidden_step, 0)

    def down_step(owner, c):
        out_ref[owner, c] = jnp.dot(
            hidden[owner, c], down[...], preferred_element_type=f32
        ).astype(bf16)

    def own_down(c, carry):
        down_step(me, c)
        return carry

    lax.fori_loop(0, chunk_count, own_down, 0)

    def peer_down(s, carry):
        c = s // (n - 1)
        d = peer(1 + s % (n - 1))
        hid_copy(d, d, c).wait_recv()
        down_step(d, c)
        return carry

    lax.fori_loop(0, chunk_count * (n - 1), peer_down, 0)

    def drain(s, carry):
        c = s // (n - 1)
        d = peer(1 + s % (n - 1))
        part_copy(d, d, me, c).wait_send()
        hid_copy(d, me, c).wait_send()
        return carry

    lax.fori_loop(0, chunk_count * (n - 1), drain, 0)


def plane_terms(x, gate, up, down, n):
    rows, kslice = x.shape
    units = gate.shape[1]
    width = down.shape[1]
    ch = rows // (n * chunk_count)
    sems = pltpu.SemaphoreType.DMA
    call = pl.pallas_call(
        lambda *refs: plane_kernel(n, *refs),
        out_shape=jax.ShapeDtypeStruct((n, chunk_count, ch, width), bf16),
        in_specs=[pl.BlockSpec(memory_space=pl.ANY)] * 4,
        out_specs=pl.BlockSpec(memory_space=pltpu.VMEM),
        scratch_shapes=[
            pltpu.VMEM((n, chunk_count, ch, kslice), bf16),
            pltpu.VMEM((kslice, units), bf16),
            pltpu.VMEM((kslice, units), bf16),
            pltpu.VMEM((units, width), bf16),
            pltpu.VMEM((n, chunk_count, 2, ch, units), bf16),
            pltpu.VMEM((chunk_count, 2, ch, units), f32),
            pltpu.VMEM((n, chunk_count, 2, ch, units), bf16),
            pltpu.VMEM((n, chunk_count, ch, units), bf16),
            sems((4,)),
            sems((n, chunk_count)),
            sems((n, chunk_count)),
            sems((n, chunk_count)),
            sems((n, chunk_count)),
        ],
        compiler_params=pltpu.CompilerParams(
            collective_id=0, has_side_effects=True, vmem_limit_bytes=48 * 1024 * 1024
        ),
        cost_estimate=pl.CostEstimate(
            flops=80_000_000_000, bytes_accessed=100_000_000, transcendentals=0
        ),
        name="plane",
    )
    out = call(x.reshape(n, chunk_count, ch, kslice), gate, up, down)
    return out.reshape(rows, width)


def on_device(
    tokens, norm_gain, spill_blocks, image_gate, image_up, image_down, text_gate, text_up, text_down
):
    rows, width = tokens.shape
    n_tp = lax.axis_size("tp")
    n_grp = lax.axis_size("grp")
    group = lax.axis_index("grp")
    n_spill = spill_blocks.shape[0]
    in_text = group == n_grp - 1
    kslice = image_gate.shape[0]
    wide = tokens.astype(f32)
    scale = lax.rsqrt(jnp.mean(wide * wide, axis=-1, keepdims=True) + norm_epsilon)
    normed = (wide * scale * norm_gain).astype(bf16)

    cols = normed.reshape(rows, n_grp, kslice).transpose(1, 0, 2)
    cols = lax.all_to_all(cols, "grp", 0, 0, tiled=True)
    cols = lax.all_gather(cols, "tp", axis=1, tiled=False)
    image_part = cols[: n_grp - 1].reshape(-1, kslice)
    spill_part = cols[n_grp - 1][spill_blocks].reshape(-1, kslice)
    x = jnp.concatenate([image_part, spill_part], axis=0)
    n_rows = x.shape[0]
    step = 16 * n_grp * chunk_count
    padded = (n_rows + step - 1) // step * step
    x = jnp.pad(x, ((0, padded - n_rows), (0, 0)))
    terms = plane_terms(x, image_gate, image_up, image_down, n_grp)

    piece = lax.all_gather(normed, "tp", axis=0, tiled=True)

    def text_ffn():
        g = jnp.dot(piece, text_gate, preferred_element_type=f32)
        u = jnp.dot(piece, text_up, preferred_element_type=f32)
        h = (jax.nn.silu(g) * u).astype(bf16)
        return jnp.dot(h, text_down, preferred_element_type=f32).astype(bf16)

    text_terms = lax.cond(
        in_text, text_ffn, lambda: jnp.zeros((n_tp * rows, width), bf16)
    )
    text_out = lax.psum_scatter(text_terms, "tp", scatter_dimension=0, tiled=True)

    image_terms = terms[: (n_grp - 1) * n_tp * rows].reshape(n_grp - 1, n_tp, rows, kslice)
    spill_terms = terms[(n_grp - 1) * n_tp * rows : n_rows].reshape(n_spill, rows, kslice)
    placed = jnp.zeros((n_tp, rows, kslice), bf16).at[spill_blocks].set(spill_terms)
    every = jnp.concatenate([image_terms, placed[None]], axis=0).transpose(1, 0, 2, 3)
    mine = lax.psum_scatter(every.reshape(n_tp, -1, kslice), "tp", scatter_dimension=0, tiled=True)
    mine = mine.reshape(n_grp, rows, kslice)
    back = lax.all_to_all(mine, "grp", 0, 0, tiled=True)
    branch = back.transpose(1, 0, 2).reshape(rows, width)
    is_spill = jnp.any(lax.axis_index("tp") == spill_blocks)
    use_text = jnp.logical_and(in_text, jnp.logical_not(is_spill))
    branch = jnp.where(use_text, text_out, branch)
    return (wide + branch.astype(f32)).astype(bf16)


def solution(mesh):
    in_specs = (
        P(("grp", "tp"), None),
        P(),
        P(),
        P("grp", "tp"),
        P("grp", "tp"),
        P("tp", "grp"),
        P(None, "tp"),
        P(None, "tp"),
        P("tp", None),
    )
    out_specs = P(("grp", "tp"), None)
    return jax.shard_map(
        on_device, mesh=mesh, in_specs=in_specs, out_specs=out_specs, check_vma=False
    )
```
